32 devices in a mesh: dp: 32 (over z, y, x, core), tensor: 1.
Axes of the slice: x: 2, y: 2, z: 4, core: 2. Of those that a mesh axis runs over, the one named last changes fastest.
Arguments:
- activations: bfloat16 [384, 8192], P('dp', 'tensor'), may hold values from -400 to 400, as said below
- weight: bfloat16 [8192, 28672], P('dp', 'tensor'), may hold values from -0.0625 to 0.0625
Outputs:
- channel_mean: float32 [8192], P('dp')
- column_errors: float32 [4, 28672], P(None, ('tensor', 'dp'))
- errors: float32 [4], replicated
The draws below stay inside these ranges and needn't reach their ends.
Inputs may be any that keep to these rules, and one draw needn't show every extreme that they name: activations and weight are finite real values within the ranges stated above.
All inputs are finite; a program needn't handle non-finite values.
Results may differ from the reference program's by a relative error of at most 0.0012.
The reference program's roundings to bfloat16 on the way (of `dequant`) count: a program that leaves them out, or rounds other values in their place, can miss the bound.
Values may be sent and summed in bfloat16 or wider, within the bound.
A program may use at most 128 MiB of HBM per device.

```python
import math
import jax
import jax.numpy as jnp
from jax import lax

D = 8192
F = 28672
GROUP = 128
GRID = 4
TOKENS = 384
N_TENSOR = 1


def draw_activations(key, part):
    base_key = jax.random.fold_in(key, 11)
    key_main, key_row, key_col = jax.random.split(base_key, 3)
    position = jnp.arange(TOKENS, dtype=jnp.float32) / max(TOKENS - 1, 1)
    row_scale = jnp.exp(math.log(4.0) * position + jax.random.uniform(key_row, (TOKENS,), jnp.float32, -0.3, 0.3))
    col_scale = jnp.exp(jax.random.uniform(key_col, (D,), jnp.float32, 0.0, math.log(10.0)))
    values = jnp.clip(jax.random.normal(key_main, (TOKENS, D), jnp.float32), -6.0, 6.0)
    return (values * row_scale[:, None] * col_scale[None, :]).astype(jnp.bfloat16)


def level_of(own_key, shape, cuts, smallest, top_value):
    gain, own = 1.0, jax.random.fold_in(own_key, 6)
    for axis_at, parts in cuts:
        draws = jnp.exp(jax.random.uniform(jax.random.fold_in(own, axis_at), (parts,), jnp.float32, smallest / len(cuts), top_value / len(cuts)))
        gain = gain * jnp.repeat(draws, shape[axis_at] // parts).reshape([-1 if axis == axis_at else 1 for axis in range(len(shape))])
    return gain


def scatter_about(stream_key, extent, spread, limit, cuts=(), kind=jnp.bfloat16):
    entries = spread * jax.random.normal(stream_key, extent, jnp.float32)
    if cuts:
        entries = entries * level_of(stream_key, extent, cuts, -0.22, 0.18)
    return jnp.clip(entries, -limit, limit).astype(kind)


def setup_inputs(seed: int = 0) -> dict:
    splits = jax.random.split(jax.random.key(seed), 3)
    return {
        "activations": draw_activations(jax.random.fold_in(splits[2], 71), 0),
        "weight": scatter_about(splits[1], (D, F), D ** -0.5, 0.0625, ((0, 32),)),
    }


def soft_round(values):
    return values - jnp.sin(2.0 * math.pi * values) / (2.0 * math.pi)

def scale_table(channel_mean):
    ratios = jnp.arange(GRID, dtype=jnp.float32) / GRID
    raw = jnp.exp(ratios[:, None] * jnp.log(channel_mean)[None, :])
    top = lax.optimization_barrier(jnp.max(raw, axis=1, keepdims=True))
    bottom = lax.optimization_barrier(jnp.min(raw, axis=1, keepdims=True))
    return raw / jnp.sqrt(top * bottom)

def block_errors(activations, block, scales):
    base_out = jnp.dot(activations, block, preferred_element_type=jnp.float32)
    width = block.shape[1]
    weight_float = block.astype(jnp.float32)

    def one_ratio(factor):
        scaled = weight_float * factor[:, None]
        grouped = scaled.reshape(D // GROUP, GROUP, width)
        quant_step = (lax.optimization_barrier(jnp.max(jnp.abs(grouped), axis=1, keepdims=True)) + 1e-06) / 7.0
        levels = soft_round(grouped / quant_step)
        dequant = ((levels * quant_step).reshape(D, width) / factor[:, None]).astype(jnp.bfloat16)
        quant_out = jnp.dot(activations, dequant, preferred_element_type=jnp.float32)
        residue = quant_out - base_out
        return lax.optimization_barrier(jnp.sum(residue * residue, axis=0))
    return lax.map(one_ratio, scales)

def reference(activations, weight):
    act_float = activations.astype(jnp.float32)
    channel_mean = lax.optimization_barrier(jnp.mean(jnp.abs(act_float), axis=0)) + 1e-06
    scales = scale_table(channel_mean)
    blocks = jnp.transpose(weight.reshape(D, N_TENSOR, F // N_TENSOR), (1, 0, 2))
    column_sums = lax.map(lambda block: block_errors(activations, block, scales), blocks)
    column_sums = jnp.transpose(column_sums, (1, 0, 2)).reshape(GRID, F)
    column_errors = column_sums / TOKENS
    errors = lax.optimization_barrier(jnp.sum(column_sums, axis=1)) / (TOKENS * F)
    return (channel_mean, column_errors, errors)
```

```python
import functools
import math

import jax
import jax.numpy as jnp
from jax import lax
from jax.experimental import pallas as pl
from jax.experimental.pallas import tpu as pltpu
from jax.sharding import PartitionSpec as P

GROUP = 128
GRID = 4
LANES = 128
TILE = 256
SINE = (
    6.283182818832115,
    -41.34142141640176,
    81.59618421926638,
    -76.5801034177733,
    41.205405703161745,
    -12.271277356143528,
)


def sine_of_turns(r):
    square = r * r
    value = SINE[-1] * square + SINE[-2]
    for c in SINE[-3::-1]:
        value = value * square + c
    return value * r


def partial_kernel(steps, a_ref, w_ref, s_ref, out_ref, acc, change):
    step = pl.program_id(0)
    depth, width = w_ref.shape

    @pl.when(step == 0)
    def _():
        acc[...] = jnp.zeros_like(acc)

    def tile(start, size):
        def columns(offset, length):
            if isinstance(start, int):
                return pl.ds(start + offset, length)
            return pl.ds(pl.multiple_of(start + offset, LANES), length)

        for k in range(GRID):
            for g in range(depth // GROUP):
                rows = pl.ds(g * GROUP, GROUP)
                for c in range(0, size, LANES):
                    lanes = min(LANES, size - c)
                    w = w_ref[rows, columns(c, lanes)].astype(jnp.float32)
                    scaled = w * s_ref[k, rows, :lanes]
                    top = jnp.max(jnp.abs(scaled), axis=0, keepdims=True)
                    quant_step = (top + 1e-06) / 7.0
                    v = scaled * (1.0 / quant_step)
                    wave = sine_of_turns(v - jnp.round(v))
                    wave = wave * (quant_step * (0.5 / math.pi))
                    dequant = w - wave * s_ref[GRID + k, rows, :lanes]
                    dequant = dequant.astype(jnp.bfloat16).astype(jnp.float32)
                    change[k, rows, pl.ds(c, lanes)] = (dequant - w).astype(jnp.bfloat16)
            acc[k, :, columns(0, size)] += jnp.dot(
                a_ref[...], change[k, :, pl.ds(0, size)], preferred_element_type=jnp.float32
            )

    whole = width // TILE
    if whole:

        @pl.loop(0, whole)
        def _(i):
            tile(i * TILE, TILE)

    if width % TILE:
        tile(whole * TILE, width % TILE)

    @pl.when(step == steps - 1)
    def _():
        for k in range(GRID):
            out_ref[k] = acc[k].astype(out_ref.dtype)


def partial_residue(tokens, columns, table, depth, kind):
    count, channels = tokens.shape
    width = columns.shape[1]
    steps = channels // depth
    return pl.pallas_call(
        functools.partial(partial_kernel, steps),
        grid=(steps,),
        out_shape=jax.ShapeDtypeStruct((GRID, count, width), kind),
        in_specs=[
            pl.BlockSpec((count, depth), lambda i: (0, i)),
            pl.BlockSpec((depth, width), lambda i: (i, 0)),
            pl.BlockSpec((2 * GRID, depth, LANES), lambda i: (0, i, 0)),
        ],
        out_specs=pl.BlockSpec((GRID, count, width), lambda i: (0, 0, 0)),
        scratch_shapes=[
            pltpu.VMEM((GRID, count, width), jnp.float32),
            pltpu.VMEM((GRID, depth, min(TILE, -(-width // LANES) * LANES)), jnp.bfloat16),
        ],
        compiler_params=pltpu.CompilerParams(
            dimension_semantics=("arbitrary",), vmem_limit_bytes=48 << 20
        ),
        cost_estimate=pl.CostEstimate(
            flops=30 * GRID * channels * width * 16,
            bytes_accessed=4 * channels * width,
            transcendentals=0,
        ),
    )(tokens, columns, table)


def on_device(activations, weight):
    n = lax.axis_size("dp")
    half = n // 2
    me = lax.axis_index("dp")
    side, place = me // half, me % half
    groups = [list(range(half)), list(range(half, n))]
    across = [(i, (i + half) % n) for i in range(n)]

    widened = lax.all_gather(activations, "tensor", axis=1, tiled=True)
    own_tokens, channels = widened.shape
    mine = channels // 2
    token_count = own_tokens * n
    kept = lax.dynamic_slice_in_dim(widened, side * mine, mine, axis=1)
    away = lax.dynamic_slice_in_dim(widened, (1 - side) * mine, mine, axis=1)
    other = lax.ppermute(away, "dp", across)
    first = side == 0
    pair = jnp.concatenate([jnp.where(first, kept, other), jnp.where(first, other, kept)], axis=0)
    tokens = lax.all_gather(pair, "dp", axis=0, tiled=True, axis_index_groups=groups)

    width = weight.shape[1]
    away_weight = lax.dynamic_slice_in_dim(weight, (1 - side) * (width // 2), width // 2, axis=1)
    kept_weight = lax.dynamic_slice_in_dim(weight, side * (width // 2), width // 2, axis=1)
    exchange = functools.partial(
        lax.all_to_all, axis_name="dp", split_axis=1, concat_axis=0, tiled=True, axis_index_groups=groups
    )
    away_columns = exchange(away_weight)
    kept_columns = exchange(kept_weight)

    half_mean = jnp.sum(jnp.abs(tokens.astype(jnp.float32)), axis=0) / token_count + 1e-06
    other_mean = lax.ppermute(half_mean, "dp", across)
    ratios = jnp.arange(GRID, dtype=jnp.float32) / GRID
    raw = jnp.exp(ratios[:, None] * jnp.log(half_mean)[None, :])
    raw_other = jnp.exp(ratios[:, None] * jnp.log(other_mean)[None, :])
    top = jnp.maximum(jnp.max(raw, axis=1, keepdims=True), jnp.max(raw_other, axis=1, keepdims=True))
    bottom = jnp.minimum(jnp.min(raw, axis=1, keepdims=True), jnp.min(raw_other, axis=1, keepdims=True))
    scales = raw / jnp.sqrt(top * bottom)
    table = jnp.concatenate([scales, 1.0 / scales], axis=0)
    table = jnp.broadcast_to(table[:, :, None], (2 * GRID, mine, LANES))

    depth = weight.shape[0]
    away_part = partial_residue(tokens, away_columns, table, depth, jnp.bfloat16)
    arrived = lax.ppermute(away_part, "dp", across)
    own_part = partial_residue(tokens, kept_columns, table, depth, jnp.float32)
    residue = own_part + arrived.astype(jnp.float32)
    column_sums = jnp.sum(residue * residue, axis=1)

    totals = lax.psum(jnp.sum(column_sums, axis=1), ("dp", "tensor"))
    errors = totals / (token_count * width * lax.axis_size("tensor"))
    column_errors = column_sums / token_count
    own_mean = lax.dynamic_slice_in_dim(half_mean, place * depth, depth)
    return (own_mean, column_errors, errors)


def solution(mesh):
    placed = (P("dp", "tensor"), P("dp", "tensor"))
    return jax.shard_map(
        on_device,
        mesh=mesh,
        in_specs=placed,
        out_specs=(P("dp"), P(None, ("tensor", "dp")), P()),
        check_vma=False,
    )
```
